16 devices in a mesh: rep: 2 (over y, z), dp: 8 (over x, core).
Axes of the slice: x: 4, y: 2, z: 1, core: 2. Of those that a mesh axis runs over, the one named last changes fastest.
The devices are a block of a 4x4x8 slice.
Arguments:
- x: bfloat16 [16, 2048, 768], P(('rep', 'dp')), parts along dimension 0
- dy: bfloat16 [16, 2048, 768], P(('rep', 'dp')), parts along dimension 0
- wq: bfloat16 [2, 768, 1024], P(None, 'dp')
- wk: bfloat16 [2, 768, 1024], P(None, 'dp')
- wv: bfloat16 [2, 768, 1024], P(None, 'dp')
- wo: bfloat16 [2, 1024, 768], P(None, 'dp')
- w_gate: bfloat16 [2, 768, 6144], P(None, 'dp')
- w_up: bfloat16 [2, 768, 6144], P(None, 'dp')
- w_down: bfloat16 [2, 6144, 768], P(None, 'dp')
Outputs:
- output 1: bfloat16 [16, 2048, 768], P(('rep', 'dp')), parts along dimension 0
- output 2: bfloat16 [4, 768, 1024], P('rep', 'dp'), parts along dimension 0
- output 3: bfloat16 [4, 768, 1024], P('rep', 'dp'), parts along dimension 0
- output 4: bfloat16 [4, 768, 1024], P('rep', 'dp'), parts along dimension 0
- output 5: bfloat16 [4, 1024, 768], P('rep', 'dp'), parts along dimension 0
- output 6: bfloat16 [4, 768, 6144], P('rep', 'dp'), parts along dimension 0
- output 7: bfloat16 [4, 768, 6144], P('rep', 'dp'), parts along dimension 0
- output 8: bfloat16 [4, 6144, 768], P('rep', 'dp'), parts along dimension 0
There are 2 independent parts. The reference program is written for one: setup_inputs(seed, part) draws one part's arguments, and reference() takes and returns one part's arrays. A program takes and returns all parts, laid end to end along the dimension named above; an argument that names none is the same for every part.
All inputs are finite; a program needn't handle non-finite values.
Results may differ from the reference program's by a relative error of at most 0.027.
Values are sent between devices in bfloat16 or wider.
A program may use at most 768 MiB of HBM per device.

```python
import jax
import jax.numpy as jnp
from jax import lax

SEQUENCES = 8
TOKENS = 2048
D = 768
HEADS = 4
KV_HEADS = 4
HEAD = 256
FF = 6144
LAYERS = 2
THETA = 10000
NAMES = ("wq", "wk", "wv", "wo", "w_gate", "w_up", "w_down")
SHAPES = {
    "wq": (LAYERS, D, HEADS * HEAD),
    "wk": (LAYERS, D, KV_HEADS * HEAD),
    "wv": (LAYERS, D, KV_HEADS * HEAD),
    "wo": (LAYERS, HEADS * HEAD, D),
    "w_gate": (LAYERS, D, FF),
    "w_up": (LAYERS, D, FF),
    "w_down": (LAYERS, FF, D),
}


def bump(key, n, height):
    away = (jnp.arange(n, dtype=jnp.int32) - jax.random.randint(key, (), 0, n, jnp.int32)) % n
    return jnp.where(away < n // 8, height, 1.0)


def together(key, own, strength):
    shared = jax.random.normal(key, own.shape[1:], jnp.float32)
    return (own + strength * shared) * lax.rsqrt(1 + strength * strength)


def setup_inputs(seed: int = 0, part: int = 0) -> dict:
    kx, kdy, ka, kb, kz, kf, kh, kl, *keys = jax.random.split(jax.random.key(seed), 8 + 3 * len(NAMES))
    kx, kdy, ka, kb = (jax.random.fold_in(k, part) for k in (kx, kdy, ka, kb))
    kw, km, kv = (keys[i::3] for i in range(3))
    shape = (SEQUENCES, TOKENS, D)
    much_x, much_dy = jax.random.uniform(kz, (2,), jnp.float32, 0.0, 1.0)
    loud = 2.0 ** jax.random.uniform(jax.random.fold_in(kz, 1), (), jnp.float32, -1.0, 2.0)
    layers = 2.0 ** jax.random.uniform(kl, (LAYERS, 1, 1), jnp.float32, -1.0, 1.0)
    times = {"wq": 1.0, "wk": 1.0, "wv": 2.0, "wo": layers, "w_gate": 1.0, "w_up": bump(kh, FF, 4.0), "w_down": layers}
    x = together(ka, jax.random.normal(kx, shape, jnp.float32), much_x) * bump(kf, D, 4.0)
    dy = together(kb, jax.random.normal(kdy, shape, jnp.float32), much_dy)
    drawn = {"x": x.astype(jnp.bfloat16), "dy": (loud * dy * (SEQUENCES * TOKENS) ** -0.5).astype(jnp.bfloat16)}
    for key, name in zip(kw, NAMES, strict=True):
        drawn[name] = (jax.random.normal(key, SHAPES[name], jnp.float32) * SHAPES[name][1] ** -0.5 * times[name]).astype(jnp.bfloat16)
    return drawn


def matmul(a, w):
    return jnp.dot(a, w, preferred_element_type=jnp.float32).astype(jnp.bfloat16)


def normed(h):
    wide = h.astype(jnp.float32)
    scale = lax.rsqrt(jnp.mean(wide**2, -1, keepdims=True) + 1e-6)
    return (wide * scale).astype(jnp.bfloat16)


def turned(t, theta):
    half = t.shape[-1] // 2
    angle = jnp.arange(t.shape[0], dtype=jnp.float32)[:, None] * theta ** (-jnp.arange(half, dtype=jnp.float32) / half)
    cos, sin = jnp.cos(angle)[:, None], jnp.sin(angle)[:, None]
    a, b = t[..., :half].astype(jnp.float32), t[..., half:].astype(jnp.float32)
    return jnp.concatenate([a * cos - b * sin, b * cos + a * sin], -1).astype(jnp.bfloat16)


def seen_by(q, k, v):
    tokens, kv = q.shape[0], k.shape[1]
    q = q.reshape(tokens, kv, -1, q.shape[-1])
    scores = jnp.einsum("tgsd,ugd->gstu", q.astype(jnp.float32), k.astype(jnp.float32)) * q.shape[-1] ** -0.5
    place = jnp.arange(tokens)
    weights = jax.nn.softmax(jnp.where(place[:, None] >= place, scores, -jnp.inf), -1).astype(jnp.bfloat16)
    return jnp.einsum("gstu,ugd->tgsd", weights.astype(jnp.float32), v.astype(jnp.float32)).astype(jnp.bfloat16).reshape(tokens, -1)


def layer(h, w):
    a = normed(h)
    q, k = (turned(matmul(a, w[name]).reshape(h.shape[0], -1, HEAD), THETA) for name in ("wq", "wk"))
    h = h + matmul(seen_by(q, k, matmul(a, w["wv"]).reshape(h.shape[0], -1, HEAD)), w["wo"])
    b = normed(h)
    gate = jnp.dot(b, w["w_gate"], preferred_element_type=jnp.float32)
    up = jnp.dot(b, w["w_up"], preferred_element_type=jnp.float32)
    return h + matmul((jax.nn.silu(gate) * up).astype(jnp.bfloat16), w["w_down"])


def stack(weights, h):
    return lax.scan(lambda h, w: (layer(h, w), None), h, weights)[0]


def reference(x, dy, wq, wk, wv, wo, w_gate, w_up, w_down):
    weights = dict(zip(NAMES, (wq, wk, wv, wo, w_gate, w_up, w_down), strict=True))

    def take(so_far, sequence):
        h, by_y = sequence
        _, back = jax.vjp(stack, weights, h)
        by_weights, by_h = back(by_y)
        return jax.tree.map(lambda total, term: total + term.astype(jnp.float32), so_far, by_weights), by_h

    none_yet = {name: jnp.zeros(w.shape, jnp.float32) for name, w in weights.items()}
    by_weights, by_x = lax.scan(take, none_yet, (x, dy))
    return (by_x, *(by_weights[name].astype(jnp.bfloat16) for name in NAMES))
```

```python
import functools

import jax
import jax.numpy as jnp
from jax import lax
from jax.experimental import pallas as pl
from jax.experimental.pallas import tpu as pltpu
from jax.sharding import PartitionSpec as P

NEG = -1e30
HIDDEN = 2 * NEG
LOG2E = 1.4426950408889634
VMEM = 58 * 2**20
STRIP = 512
HEAD = 256
THETA = 10000
TILE = 512
ROWS = 512
F32, BF16 = jnp.float32, jnp.bfloat16


def _dot(a, b, ca, cb):
    return lax.dot_general(a, b, (((ca,), (cb,)), ((), ())), preferred_element_type=F32)


def _cost(flops, nbytes, exps=0):
    return pl.CostEstimate(flops=int(flops), transcendentals=int(exps), bytes_accessed=int(nbytes))


def _params(*semantics):
    return pltpu.CompilerParams(dimension_semantics=semantics, vmem_limit_bytes=VMEM)


def _whole(shape):
    return pl.BlockSpec(shape, lambda *_: (0,) * len(shape), pipeline_mode=pl.Buffered(1))


def _pieces(tokens):
    return [slice(r, min(r + ROWS, tokens)) for r in range(0, tokens, ROWS)]


def _norm_into(h_ref, n_s, nt_ref):
    for r in _pieces(h_ref.shape[0]):
        wide = h_ref[r, :].astype(F32)
        n = (wide * lax.rsqrt(jnp.mean(wide * wide, -1, keepdims=True) + 1e-6)).astype(BF16)
        n_s[r, :] = n
        nt_ref[:, r] = n.T


def _norm_back(h_ref, d_ref, dn_s, out_ref):
    for r in _pieces(h_ref.shape[0]):
        wide = h_ref[r, :].astype(F32)
        dn = dn_s[r, :].astype(BF16).astype(F32)
        scale = lax.rsqrt(jnp.mean(wide * wide, -1, keepdims=True) + 1e-6)
        mean = jnp.mean(dn * wide, -1, keepdims=True)
        by_h = (scale * (dn - wide * (scale * scale * mean))).astype(BF16)
        out_ref[r, :] = (d_ref[r, :].astype(F32) + by_h.astype(F32)).astype(BF16)


def _qkv_kernel(h_ref, w_ref, cos_ref, sin_ref, out_ref, at_ref, a_s, *, turned):
    j = pl.program_id(0)

    @pl.when(j == 0)
    def _():
        _norm_into(h_ref, a_s, at_ref)

    half = HEAD // 2
    for r in _pieces(h_ref.shape[0]):
        y = _dot(a_s[r, :], w_ref[...], 1, 0).astype(BF16)
        cos, sin = cos_ref[r, :], sin_ref[r, :]
        for at in range(0, y.shape[1], HEAD):
            a, b = y[:, at : at + half].astype(F32), y[:, at + half : at + HEAD].astype(F32)
            out_ref[r, at : at + half] = jnp.where(j < turned, a * cos - b * sin, a).astype(BF16)
            out_ref[r, at + half : at + HEAD] = jnp.where(j < turned, b * cos + a * sin, b).astype(BF16)


def project(h, w, cos, sin, width):
    tokens, d = h.shape
    tile = 2 * HEAD
    return pl.pallas_call(
        functools.partial(_qkv_kernel, turned=2 * width // tile),
        grid=(3 * width // tile,),
        in_specs=[_whole((tokens, d)), pl.BlockSpec((d, tile), lambda j: (0, j)), _whole(cos.shape), _whole(sin.shape)],
        out_specs=[pl.BlockSpec((tokens, tile), lambda j: (0, j)), _whole((d, tokens))],
        out_shape=[jax.ShapeDtypeStruct((tokens, 3 * width), BF16), jax.ShapeDtypeStruct((d, tokens), BF16)],
        scratch_shapes=[pltpu.VMEM((tokens, d), BF16)],
        compiler_params=_params("arbitrary"),
        cost_estimate=_cost(2 * tokens * d * 3 * width, 2 * (2 * tokens * d + 3 * d * width + 3 * tokens * width)),
        name="qkv_forward",
    )(h, w, cos, sin)


def _choose(refs, per, j, run):
    for n, ref in enumerate(refs):

        @pl.when((j >= n * per) & (j < (n + 1) * per))
        def _():
            run(ref)


def _qkv_weights_kernel(at_ref, *rest, per):
    *cs, out_ref = rest

    def run(c_ref):
        out_ref[...] = _dot(at_ref[...], c_ref[...], 1, 0).astype(BF16)

    _choose(cs, per, pl.program_id(0), run)


def _thirds(tokens, tile, per):
    return [pl.BlockSpec((tokens, tile), lambda j, n=n: (0, jnp.clip(j - n * per, 0, per - 1))) for n in range(3)]


def project_weights(at, parts):
    d, tokens = at.shape
    width, tile = parts[0].shape[1], 512
    per = width // tile
    return pl.pallas_call(
        functools.partial(_qkv_weights_kernel, per=per),
        grid=(3 * per,),
        in_specs=[_whole((d, tokens)), *_thirds(tokens, tile, per)],
        out_specs=pl.BlockSpec((d, tile), lambda j: (0, j)),
        out_shape=jax.ShapeDtypeStruct((d, 3 * width), BF16),
        compiler_params=_params("arbitrary"),
        cost_estimate=_cost(2 * tokens * d * 3 * width, 2 * (tokens * d + 3 * d * width + 3 * tokens * width)),
        name="qkv_weights",
    )(at, *parts)


def _qkv_input_kernel(h_ref, d_ref, w_ref, *rest, per):
    *cs, out_ref, da_s = rest
    j = pl.program_id(0)

    @pl.when(j == 0)
    def _():
        da_s[...] = jnp.zeros_like(da_s)

    def run(c_ref):
        for r in _pieces(h_ref.shape[0]):
            da_s[r, :] += _dot(c_ref[r, :], w_ref[...], 1, 1)

    _choose(cs, per, j, run)

    @pl.when(j == pl.num_programs(0) - 1)
    def _():
        _norm_back(h_ref, d_ref, da_s, out_ref)


def project_input(h, d_h, w, parts):
    tokens, d = h.shape
    width, tile = parts[0].shape[1], 512
    per = width // tile
    return pl.pallas_call(
        functools.partial(_qkv_input_kernel, per=per),
        grid=(3 * per,),
        in_specs=[_whole((tokens, d)), _whole((tokens, d)), pl.BlockSpec((d, tile), lambda j: (0, j)), *_thirds(tokens, tile, per)],
        out_specs=_whole((tokens, d)),
        out_shape=jax.ShapeDtypeStruct((tokens, d), BF16),
        scratch_shapes=[pltpu.VMEM((tokens, d), F32)],
        compiler_params=_params("arbitrary"),
        cost_estimate=_cost(2 * tokens * d * 3 * width, 2 * (3 * tokens * d + 3 * d * width + 3 * tokens * width)),
        name="qkv_input",
    )(h, d_h, w, *parts)


def _gate_up_kernel(h_ref, w_ref, gu_ref, act_ref, bt_ref, b_s):
    @pl.when(pl.program_id(0) == 0)
    def _():
        _norm_into(h_ref, b_s, bt_ref)

    t = act_ref.shape[1]
    for r in _pieces(h_ref.shape[0]):
        both = _dot(b_s[r, :], w_ref[...], 1, 0)
        gu_ref[r, :] = both
        gate = both[:, :t]
        act_ref[r, :] = (gate * lax.logistic(gate) * both[:, t:]).astype(BF16)


def gate_up(h, w):
    tokens, d = h.shape
    ff = w.shape[1] // 2
    return pl.pallas_call(
        _gate_up_kernel,
        grid=(ff // TILE,),
        in_specs=[_whole((tokens, d)), pl.BlockSpec((d, 2 * TILE), lambda j: (0, j))],
        out_specs=[pl.BlockSpec((tokens, 2 * TILE), lambda j: (0, j)), pl.BlockSpec((tokens, TILE), lambda j: (0, j)), _whole((d, tokens))],
        out_shape=[jax.ShapeDtypeStruct((tokens, 2 * ff), F32), jax.ShapeDtypeStruct((tokens, ff), BF16),
                   jax.ShapeDtypeStruct((d, tokens), BF16)],
        scratch_shapes=[pltpu.VMEM((tokens, d), BF16)],
        compiler_params=_params("arbitrary"),
        cost_estimate=_cost(4 * tokens * d * ff, 10 * tokens * ff + 4 * d * ff, tokens * ff),
        name="gate_up",
    )(h, w)


def _hidden_back_kernel(*refs, carried, final):
    refs = list(refs)
    dh_ref, bt_ref, gu_ref, w_ref, wd_ref = refs[:5]
    del refs[:5]
    given = refs.pop(0) if carried else None
    h_ref = refs.pop(0) if final else None
    dw_ref, out_ref, dgu_s = refs[:3]
    db = refs[3] if final else out_ref
    j = pl.program_id(0)

    @pl.when(j == 0)
    def _():
        db[...] = given[...] if carried else jnp.zeros_like(db)

    t = wd_ref.shape[0]
    for r in _pieces(dh_ref.shape[0]):
        da = _dot(dh_ref[r, :], wd_ref[...], 1, 1).astype(BF16).astype(F32)
        gate, up = gu_ref[r, :t], gu_ref[r, t:]
        s = lax.logistic(gate)
        silu = gate * s
        dgu_s[r, :t] = (da * up * (s + silu * (1.0 - s))).astype(BF16)
        dgu_s[r, t:] = (da * silu).astype(BF16)
        db[r, :] += _dot(dgu_s[r, :], w_ref[...], 1, 1)
    dw_ref[...] = _dot(bt_ref[...], dgu_s[...], 1, 0).astype(BF16)

    if final:

        @pl.when(j == pl.num_programs(0) - 1)
        def _():
            _norm_back(h_ref, dh_ref, db, out_ref)


def hidden_back(dh, bt, gu, w, wd, first, count, given=None, h=None):
    tokens, d = dh.shape
    carried, final = given is not None, h is not None
    in_specs = [_whole((tokens, d)), _whole((d, tokens)), pl.BlockSpec((tokens, 2 * TILE), lambda j: (0, first + j)),
                pl.BlockSpec((d, 2 * TILE), lambda j: (0, first + j)), pl.BlockSpec((TILE, d), lambda j: (first + j, 0))]
    args = [dh, bt, gu, w, wd]
    if carried:
        in_specs.append(_whole((tokens, d)))
        args.append(given)
    if final:
        in_specs.append(_whole((tokens, d)))
        args.append(h)
    n = count * TILE
    return pl.pallas_call(
        functools.partial(_hidden_back_kernel, carried=carried, final=final),
        grid=(count,),
        in_specs=in_specs,
        out_specs=[pl.BlockSpec((d, 2 * TILE), lambda j: (0, j)), _whole((tokens, d))],
        out_shape=[jax.ShapeDtypeStruct((d, 2 * n), BF16), jax.ShapeDtypeStruct((tokens, d), BF16 if final else F32)],
        scratch_shapes=[pltpu.VMEM((tokens, 2 * TILE), BF16)] + ([pltpu.VMEM((tokens, d), F32)] if final else []),
        compiler_params=_params("arbitrary"),
        cost_estimate=_cost(10 * tokens * d * n, 8 * tokens * n + 10 * d * n + 6 * tokens * d, tokens * n),
        name="hidden_back",
    )(*args)


def _alternate_kernel(a_ref, b_ref, out_ref):
    for n in range(a_ref.shape[1] // TILE):
        at = n * TILE
        out_ref[:, 2 * at : 2 * at + TILE] = a_ref[:, at : at + TILE]
        out_ref[:, 2 * at + TILE : 2 * at + 2 * TILE] = b_ref[:, at : at + TILE]


def alternate(a, b, number):
    _, rows, ff = a.shape
    wide = ff // 2
    return pl.pallas_call(
        _alternate_kernel,
        grid=(ff // wide,),
        in_specs=[pl.BlockSpec((None, rows, wide), lambda j: (number, 0, j))] * 2,
        out_specs=pl.BlockSpec((rows, 2 * wide), lambda j: (0, j)),
        out_shape=jax.ShapeDtypeStruct((rows, 2 * ff), a.dtype),
        compiler_params=_params("arbitrary"),
        cost_estimate=_cost(rows * ff, 8 * rows * ff),
        name="alternate",
    )(a, b)


def _part_kernel(*refs):
    *ins, a_ref, b_ref = refs
    for n, ref in enumerate(ins):
        for m in range(a_ref.shape[2] // TILE):
            at = m * TILE
            a_ref[n, :, at : at + TILE] = ref[:, 2 * at : 2 * at + TILE]
            b_ref[n, :, at : at + TILE] = ref[:, 2 * at + TILE : 2 * at + 2 * TILE]


def part(pairs):
    rows, both = pairs[0].shape
    wide = both // 4
    return pl.pallas_call(
        _part_kernel,
        grid=(2,),
        in_specs=[pl.BlockSpec((rows, 2 * wide), lambda j: (0, j))] * len(pairs),
        out_specs=[pl.BlockSpec((len(pairs), rows, wide), lambda j: (0, 0, j))] * 2,
        out_shape=[jax.ShapeDtypeStruct((len(pairs), rows, both // 2), pairs[0].dtype)] * 2,
        compiler_params=_params("arbitrary"),
        cost_estimate=_cost(rows * both, 4 * rows * both * len(pairs)),
        name="part",
    )(*pairs)


def _gap(bk, bq):
    return lax.broadcasted_iota(jnp.int32, (bk, bq), 1) - lax.broadcasted_iota(jnp.int32, (bk, bq), 0)


def _attend_kernel(q_ref, k_ref, v_ref, o_ref, lse_ref, top_s, mix_s, gap_s, *, kb, bq, bk):
    d = HEAD
    iq = pl.program_id(1)
    scale = d**-0.5
    e = scale * LOG2E
    wide = min(STRIP, bq)
    pieces = [(i, at) for i in range(kb) for at in range(0, bq, wide)]

    @pl.when(iq == 0)
    def _():
        gap_s[...] = _gap(bk, bq)

    for i in range(kb):
        top_s[i : i + 1, :] = jnp.full((1, bq), NEG, F32)
        mix_s[i] = jnp.zeros((d + 8, bq), F32)
    ones = jnp.ones((8, bk), BF16)

    def block(j, masked):
        here = pl.ds(j * bk, bk)
        scores = [_dot(k_ref[here, i * d : (i + 1) * d], q_ref[at : at + wide, i * d : (i + 1) * d], 1, 1) for i, at in pieces]
        ok = gap_s[...] >= j * bk - iq * bq if masked else None
        weights, keeps = [], []
        for (i, at), s in zip(pieces, scores):
            if masked:
                s = jnp.where(ok[:, at : at + wide], s, HIDDEN)
            old = top_s[i : i + 1, at : at + wide]
            top = jnp.maximum(old, s.max(axis=0, keepdims=True))
            top_s[i : i + 1, at : at + wide] = top
            weights.append(jnp.exp2((s - top) * e).astype(BF16))
            keeps.append(jnp.exp2((old - top) * e))
        for (i, at), p, keep in zip(pieces, weights, keeps):
            values = jnp.concatenate([v_ref[here, i * d : (i + 1) * d].T, ones], axis=0)
            mix_s[i, :, at : at + wide] = mix_s[i, :, at : at + wide] * keep + _dot(values, p, 1, 0)

    first = iq * (bq // bk)
    lax.fori_loop(0, first, lambda j, _: block(j, False), None)
    lax.fori_loop(first, first + bq // bk, lambda j, _: block(j, True), None)
    for i in range(kb):
        top, total = top_s[i : i + 1, :], mix_s[i, d : d + 1, :]
        o_ref[:, i * d : (i + 1) * d] = (mix_s[i, :d, :] * (1 / total)).T.astype(o_ref.dtype)
        lse_ref[i] = top * scale + jnp.log(total)


def attend(qkv, width):
    tokens = qkv.shape[0]
    kb, bq, bk = width // HEAD, 1024, 512
    wide = kb * HEAD
    n = width // wide
    return pl.pallas_call(
        functools.partial(_attend_kernel, kb=kb, bq=bq, bk=bk),
        grid=(n, tokens // bq),
        in_specs=[pl.BlockSpec((bq, wide), lambda ih, iq: (iq, ih)), pl.BlockSpec((tokens, wide), lambda ih, iq: (0, n + ih)),
                  pl.BlockSpec((tokens, wide), lambda ih, iq: (0, 2 * n + ih))],
        out_specs=[pl.BlockSpec((bq, wide), lambda ih, iq: (iq, ih)), pl.BlockSpec((kb, 1, bq), lambda ih, iq: (ih, 0, iq))],
        out_shape=[jax.ShapeDtypeStruct((tokens, width), BF16), jax.ShapeDtypeStruct((width // HEAD, 1, tokens), F32)],
        scratch_shapes=[pltpu.VMEM((kb, bq), F32), pltpu.VMEM((kb, HEAD + 8, bq), F32), pltpu.VMEM((bk, bq), jnp.int32)],
        compiler_params=_params("arbitrary", "arbitrary"),
        cost_estimate=_cost(4 * width * tokens * tokens, 8 * tokens * width, width // HEAD * tokens * tokens),
        name="attend",
    )(qkv, qkv, qkv)


def _unturn(t, cos, sin):
    half = t.shape[1] // 2
    t = t.astype(BF16).astype(F32)
    a, b = t[:, :half], t[:, half:]
    return jnp.concatenate([(a * cos + b * sin).astype(BF16), (b * cos - a * sin).astype(BF16)], axis=1)


def _attend_back_kernel(q_ref, k_ref, v_ref, o_ref, do_ref, lse_ref, cos_ref, sin_ref, dq_ref, dk_ref, dv_ref, dq_s, dk_s, dv_s, gap_s,
                        *, kb, bq, bk):
    d = HEAD
    iq = pl.program_id(1)
    scale = d**-0.5
    e = scale * LOG2E
    wide = min(STRIP, bq)
    pieces = [(i, at) for i in range(kb) for at in range(0, bq, wide)]

    @pl.when(iq == 0)
    def _():
        gap_s[...] = _gap(bk, bq)
        dk_s[...] = jnp.zeros_like(dk_s)
        dv_s[...] = jnp.zeros_like(dv_s)

    dq_s[...] = jnp.zeros_like(dq_s)
    lses = [lse_ref[i] * LOG2E for i in range(kb)]
    deltas = []
    for i in range(kb):
        both = do_ref[:, i * d : (i + 1) * d].astype(F32) * o_ref[:, i * d : (i + 1) * d].astype(F32)
        deltas.append((both[:, : d // 2] + both[:, d // 2 :]).T.sum(axis=0, keepdims=True))

    def block(j, masked):
        here = pl.ds(j * bk, bk)
        qs = [q_ref[at : at + wide, i * d : (i + 1) * d] for i, at in pieces]
        dos = [do_ref[at : at + wide, i * d : (i + 1) * d] for i, at in pieces]
        scores = [_dot(k_ref[here, i * d : (i + 1) * d], x, 1, 1) for (i, _), x in zip(pieces, qs)]
        dps = [_dot(v_ref[here, i * d : (i + 1) * d], x, 1, 1) for (i, _), x in zip(pieces, dos)]
        ok = gap_s[...] >= j * bk - iq * bq if masked else None
        for n, (i, at) in enumerate(pieces):
            p = jnp.exp2(scores[n] * e - lses[i][:, at : at + wide])
            if masked:
                p = jnp.where(ok[:, at : at + wide], p, 0.0)
            ds = (p * (dps[n] - deltas[i][:, at : at + wide])).astype(BF16)
            dv_s[i, here, :] += _dot(p.astype(BF16), dos[n], 1, 0)
            dk_s[i, here, :] += _dot(ds, qs[n], 1, 0)
            dq_s[i, :, at : at + wide] += _dot(k_ref[here, i * d : (i + 1) * d].T, ds, 1, 0)

    first = iq * (bq // bk)
    lax.fori_loop(0, first, lambda j, _: block(j, False), None)
    lax.fori_loop(first, first + bq // bk, lambda j, _: block(j, True), None)
    here = pl.ds(iq * bq, bq)
    for i in range(kb):
        dq_ref[:, i * d : (i + 1) * d] = _unturn((dq_s[i] * scale).T, cos_ref[here, :], sin_ref[here, :])

    @pl.when(iq == pl.num_programs(1) - 1)
    def _():
        for i in range(kb):
            for r in _pieces(dk_ref.shape[0]):
                dk_ref[r, i * d : (i + 1) * d] = _unturn(dk_s[i, r, :] * scale, cos_ref[r, :], sin_ref[r, :])
                dv_ref[r, i * d : (i + 1) * d] = dv_s[i, r, :].astype(BF16)


def attend_back(qkv, o, do, lse, cos, sin):
    tokens, width = o.shape
    kb, bq, bk = 2, 1024, 512
    wide = kb * HEAD
    n = width // wide
    queries = pl.BlockSpec((bq, wide), lambda ih, iq: (iq, ih))
    keys = pl.BlockSpec((tokens, wide), lambda ih, iq: (0, ih))
    return pl.pallas_call(
        functools.partial(_attend_back_kernel, kb=kb, bq=bq, bk=bk),
        grid=(n, tokens // bq),
        in_specs=[queries, pl.BlockSpec((tokens, wide), lambda ih, iq: (0, n + ih)), pl.BlockSpec((tokens, wide), lambda ih, iq: (0, 2 * n + ih)),
                  queries, queries, pl.BlockSpec((kb, 1, bq), lambda ih, iq: (ih, 0, iq)), _whole(cos.shape), _whole(sin.shape)],
        out_specs=[queries, keys, keys],
        out_shape=[jax.ShapeDtypeStruct((tokens, width), BF16)] * 3,
        scratch_shapes=[pltpu.VMEM((kb, HEAD, bq), F32), pltpu.VMEM((kb, tokens, HEAD), F32), pltpu.VMEM((kb, tokens, HEAD), F32),
                        pltpu.VMEM((bk, bq), jnp.int32)],
        compiler_params=_params("arbitrary", "arbitrary"),
        cost_estimate=_cost(10 * width * tokens * tokens, 16 * tokens * width, width // HEAD * tokens * tokens),
        name="attend_back",
    )(qkv, qkv, qkv, o, do, lse, cos, sin)


def matmul(a, w):
    return jnp.dot(a, w, preferred_element_type=F32).astype(BF16)


def outer(a, b):
    return _dot(a, b, 0, 0).astype(BF16)


def solution(mesh):
    gather = lambda w: lax.all_gather(w, "dp", axis=0, tiled=True)
    scatter = lambda w: lax.psum_scatter(w, "dp", scatter_dimension=0, tiled=True)
    group = mesh.shape["dp"]

    def step(x, dy, wq, wk, wv, wo, w_gate, w_up, w_down):
        layers, rows, width = wq.shape
        d, ff = wo.shape[2], w_gate.shape[2]
        h, dh = x[0], dy[0]
        tokens = h.shape[0]
        half = HEAD // 2
        angle = jnp.arange(tokens, dtype=F32)[:, None] * THETA ** (-jnp.arange(half, dtype=F32) / half)
        cos, sin = jnp.cos(angle), jnp.sin(angle)

        kept = []
        for number in range(layers):
            qkvo = gather(jnp.concatenate([wq[number], wk[number], wv[number], wo[number].reshape(rows, width)], axis=1))
            both = gather(alternate(w_gate, w_up, number))
            down = gather(w_down[number])
            out = qkvo[:, 3 * width :].reshape(width, d)
            qkv, at = project(h, qkvo, cos, sin, width)
            o, lse = attend(qkv, width)
            mid = h + matmul(o, out)
            gu, act, bt = gate_up(mid, both)
            kept.append((h, qkvo, both, down, out, qkv, at, o, lse, mid, gu, act, bt))
            h = mid + matmul(act, down)

        by_down, by_out, by_qkv = ([None] * layers for _ in range(3))
        tiles = ff // TILE
        sent = []

        def tie(*values):
            out = lax.optimization_barrier((*values, *(store[n] for store, n in sent)))
            for (store, n), got in zip(sent, out[len(values) :]):
                store[n] = got
            sent.clear()
            return out[: len(values)]

        def send(store, n, value):
            store[n] = scatter(value)
            sent.append((store, n))

        first, second = [None] * layers, [None] * layers
        cut = tiles // 2
        for number in reversed(range(layers)):
            h, qkvo, both, down, out, qkv, at, o, lse, mid, gu, act, bt = kept[number]
            by_w, dh = lax.optimization_barrier((outer(act, dh), dh))
            late, sent[:] = sent[1:], sent[:1]
            (dh,) = tie(dh)
            sent.extend(late)
            send(by_down, number, by_w)
            by_w, given = hidden_back(dh, bt, gu, both, down, 0, cut)
            (given,) = tie(given)
            send(first, number, by_w)
            by_w, d_mid = hidden_back(dh, bt, gu, both, down, cut, tiles - cut, given=given, h=mid)
            (d_mid,) = tie(d_mid)
            send(second, number, by_w)
            by_w, d_mid = lax.optimization_barrier((outer(o, d_mid), d_mid))
            do = _dot(d_mid, out, 1, 1).astype(BF16)
            parts = tie(*attend_back(qkv, o, do, lse, cos, sin))
            send(by_out, number, by_w)
            by_w, *parts = lax.optimization_barrier((project_weights(at, parts), *parts))
            send(by_qkv, number, by_w)
            dh = project_input(h, d_mid, qkvo, parts)
        by_both = [jnp.concatenate(pair, axis=1) for pair in zip(first, second)]
        by_gate, by_up = part(by_both)
        by_q, by_k, by_v = (jnp.stack([g[:, n * width : (n + 1) * width] for g in by_qkv]) for n in range(3))
        return dh[None], by_q, by_k, by_v, jnp.stack(by_out), by_gate, by_up, jnp.stack(by_down)

    states, cut = P(("rep", "dp"), None, None), P(None, "dp", None)
    return jax.shard_map(
        step,
        mesh=mesh,
        in_specs=(states, states) + (cut,) * 7,
        out_specs=(states,) + (P("rep", "dp", None),) * 7,
        check_vma=False,
    )
```

```python
import functools

import jax
import jax.numpy as jnp
from jax import lax
from jax.experimental import pallas as pl
from jax.experimental.pallas import tpu as pltpu
from jax.sharding import PartitionSpec as P

NEG = -1e30
HIDDEN = 2 * NEG
LOG2E = 1.4426950408889634
VMEM = 58 * 2**20
HEAD = 256
THETA = 10000
TILE = 512
ROWS = 512
F32, BF16 = jnp.float32, jnp.bfloat16


def _dot(a, b, ca, cb):
    return lax.dot_general(a, b, (((ca,), (cb,)), ((), ())), preferred_element_type=F32)


def _cost(flops, nbytes, exps=0):
    return pl.CostEstimate(flops=int(flops), transcendentals=int(exps), bytes_accessed=int(nbytes))


def _params(*semantics):
    return pltpu.CompilerParams(dimension_semantics=semantics, vmem_limit_bytes=VMEM)


def _whole(shape):
    return pl.BlockSpec(shape, lambda *_: (0,) * len(shape), pipeline_mode=pl.Buffered(1))


def _pieces(tokens):
    return [slice(r, min(r + ROWS, tokens)) for r in range(0, tokens, ROWS)]


def _norm_into(h_ref, n_s, nt_ref=None):
    for r in _pieces(h_ref.shape[0]):
        wide = h_ref[r, :].astype(F32)
        n = (wide * lax.rsqrt(jnp.mean(wide * wide, -1, keepdims=True) + 1e-6)).astype(BF16)
        n_s[r, :] = n
        if nt_ref is not None:
            nt_ref[:, r] = n.T


def _norm_back(h_ref, d_ref, dn_s, out_ref):
    some = 32

    def piece(i, _):
        r = pl.ds(pl.multiple_of(i * some, some), some)
        wide = h_ref[r, :].astype(F32)
        dn = dn_s[r, :].astype(BF16).astype(F32)
        scale = lax.rsqrt(jnp.mean(wide * wide, -1, keepdims=True) + 1e-6)
        mean = jnp.mean(dn * wide, -1, keepdims=True)
        by_h = (scale * (dn - wide * (scale * scale * mean))).astype(BF16)
        out_ref[r, :] = (d_ref[r, :].astype(F32) + by_h.astype(F32)).astype(BF16)

    lax.fori_loop(0, h_ref.shape[0] // some, piece, None, unroll=4)


def _qkv_kernel(h_ref, w_ref, cos_ref, sin_ref, out_ref, at_ref, a_s, *, turned):
    j = pl.program_id(0)

    @pl.when(j == 0)
    def _():
        _norm_into(h_ref, a_s, at_ref)

    half = HEAD // 2
    for r in _pieces(h_ref.shape[0]):
        y = _dot(a_s[r, :], w_ref[...], 1, 0).astype(BF16)
        cos, sin = cos_ref[r, :], sin_ref[r, :]
        for at in range(0, y.shape[1], HEAD):
            a, b = y[:, at : at + half].astype(F32), y[:, at + half : at + HEAD].astype(F32)
            out_ref[r, at : at + half] = jnp.where(j < turned, a * cos - b * sin, a).astype(BF16)
            out_ref[r, at + half : at + HEAD] = jnp.where(j < turned, b * cos + a * sin, b).astype(BF16)


def project(h, w, cos, sin, width):
    tokens, d = h.shape
    tile = 2 * HEAD
    return pl.pallas_call(
        functools.partial(_qkv_kernel, turned=2 * width // tile),
        grid=(3 * width // tile,),
        in_specs=[_whole((tokens, d)), pl.BlockSpec((d, tile), lambda j: (0, j)), _whole(cos.shape), _whole(sin.shape)],
        out_specs=[pl.BlockSpec((tokens, tile), lambda j: (0, j)), _whole((d, tokens))],
        out_shape=[jax.ShapeDtypeStruct((tokens, 3 * width), BF16), jax.ShapeDtypeStruct((d, tokens), BF16)],
        scratch_shapes=[pltpu.VMEM((tokens, d), BF16)],
        compiler_params=_params("arbitrary"),
        cost_estimate=_cost(2 * tokens * d * 3 * width, 2 * (2 * tokens * d + 3 * d * width + 3 * tokens * width)),
        name="qkv_forward",
    )(h, w, cos, sin)


def _choose(refs, per, j, run):
    for n, ref in enumerate(refs):

        @pl.when((j >= n * per) & (j < (n + 1) * per))
        def _():
            run(ref)


def _qkv_weights_kernel(at_ref, *rest, per):
    *cs, out_ref = rest

    def run(c_ref):
        out_ref[...] = _dot(at_ref[...], c_ref[...], 1, 0).astype(BF16)

    _choose(cs, per, pl.program_id(0), run)


def _thirds(tokens, tile, per):
    return [pl.BlockSpec((tokens, tile), lambda j, n=n: (0, jnp.clip(j - n * per, 0, per - 1))) for n in range(3)]


def project_weights(at, parts):
    d, tokens = at.shape
    width, tile = parts[0].shape[1], 512
    per = width // tile
    return pl.pallas_call(
        functools.partial(_qkv_weights_kernel, per=per),
        grid=(3 * per,),
        in_specs=[_whole((d, tokens)), *_thirds(tokens, tile, per)],
        out_specs=pl.BlockSpec((d, tile), lambda j: (0, j)),
        out_shape=jax.ShapeDtypeStruct((d, 3 * width), BF16),
        compiler_params=_params("arbitrary"),
        cost_estimate=_cost(2 * tokens * d * 3 * width, 2 * (tokens * d + 3 * d * width + 3 * tokens * width)),
        name="qkv_weights",
    )(at, *parts)


def _qkv_input_kernel(h_ref, d_ref, w_ref, *rest, per):
    *cs, out_ref, da_s = rest
    j = pl.program_id(0)

    @pl.when(j == 0)
    def _():
        da_s[...] = jnp.zeros_like(da_s)

    def run(c_ref):
        for r in _pieces(h_ref.shape[0]):
            da_s[r, :] += _dot(c_ref[r, :], w_ref[...], 1, 1)

    _choose(cs, per, j, run)

    @pl.when(j == pl.num_programs(0) - 1)
    def _():
        _norm_back(h_ref, d_ref, da_s, out_ref)


def project_input(h, d_h, w, parts):
    tokens, d = h.shape
    width, tile = parts[0].shape[1], 512
    per = width // tile
    return pl.pallas_call(
        functools.partial(_qkv_input_kernel, per=per),
        grid=(3 * per,),
        in_specs=[_whole((tokens, d)), _whole((tokens, d)), pl.BlockSpec((d, tile), lambda j: (0, j)), *_thirds(tokens, tile, per)],
        out_specs=_whole((tokens, d)),
        out_shape=jax.ShapeDtypeStruct((tokens, d), BF16),
        scratch_shapes=[pltpu.VMEM((tokens, d), F32)],
        compiler_params=_params("arbitrary"),
        cost_estimate=_cost(2 * tokens * d * 3 * width, 2 * (3 * tokens * d + 3 * d * width + 3 * tokens * width)),
        name="qkv_input",
    )(h, d_h, w, *parts)


def _gate_up_kernel(h_ref, w_ref, *rest, more):
    gu_ref, act_ref, bt_ref, b_s = (*rest[1:3], None, rest[3]) if more else rest

    @pl.when(pl.program_id(0) == 0)
    def _():
        _norm_into(h_ref, b_s, bt_ref)

    t = act_ref.shape[1]
    for r in _pieces(h_ref.shape[0]):
        both = _dot(b_s[r, :], w_ref[...], 1, 0)
        gu_ref[r, :] = both
        gate = both[:, :t]
        act_ref[r, :] = (gate * lax.logistic(gate) * both[:, t:]).astype(BF16)


def gate_up(h, w, ff, act=None):
    tokens, d = h.shape
    count, more = w.shape[1] // (2 * TILE), act is not None
    first = ff // TILE - count if more else 0
    return pl.pallas_call(
        functools.partial(_gate_up_kernel, more=more),
        grid=(count,),
        in_specs=[_whole((tokens, d)), pl.BlockSpec((d, 2 * TILE), lambda j: (0, j))] + ([pl.BlockSpec(memory_space=pl.ANY)] if more else []),
        out_specs=[pl.BlockSpec((tokens, 2 * TILE), lambda j: (0, j)), pl.BlockSpec((tokens, TILE), lambda j: (0, first + j))]
        + ([] if more else [_whole((d, tokens))]),
        out_shape=[jax.ShapeDtypeStruct((tokens, w.shape[1]), F32), jax.ShapeDtypeStruct((tokens, ff), BF16)]
        + ([] if more else [jax.ShapeDtypeStruct((d, tokens), BF16)]),
        scratch_shapes=[pltpu.VMEM((tokens, d), BF16)],
        input_output_aliases={2: 1} if more else {},
        compiler_params=_params("arbitrary"),
        cost_estimate=_cost(2 * tokens * d * w.shape[1], 5 * tokens * w.shape[1] + 2 * d * w.shape[1], tokens * w.shape[1] // 2),
        name="gate_up",
    )(h, w, *([act] if more else []))


def _hidden_back_kernel(*refs, carried, final):
    refs = list(refs)
    dh_ref, bt_ref, gu_ref, w_ref, wd_ref = refs[:5]
    del refs[:5]
    given = refs.pop(0) if carried else None
    h_ref = refs.pop(0) if final else None
    dw_ref, out_ref, dgu_s = refs[:3]
    db = refs[3] if final else out_ref
    j = pl.program_id(0)

    @pl.when(j == 0)
    def _():
        db[...] = given[...] if carried else jnp.zeros_like(db)

    t = wd_ref.shape[0]
    for r in _pieces(dh_ref.shape[0]):
        da = _dot(dh_ref[r, :], wd_ref[...], 1, 1).astype(BF16).astype(F32)
        gate, up = gu_ref[r, :t], gu_ref[r, t:]
        s = lax.logistic(gate)
        silu = gate * s
        dgu_s[r, :t] = (da * up * (s + silu * (1.0 - s))).astype(BF16)
        dgu_s[r, t:] = (da * silu).astype(BF16)
        db[r, :] += _dot(dgu_s[r, :], w_ref[...], 1, 1)
    dw_ref[...] = _dot(bt_ref[...], dgu_s[...], 1, 0).astype(BF16)

    if final:

        @pl.when(j == pl.num_programs(0) - 1)
        def _():
            _norm_back(h_ref, dh_ref, db, out_ref)


def hidden_back(dh, bt, gu, w, wd, first, down, count, room=0, given=None, h=None):
    tokens, d = dh.shape
    carried, final = given is not None, h is not None
    in_specs = [_whole((tokens, d)), _whole((d, tokens)), pl.BlockSpec((tokens, 2 * TILE), lambda j: (0, first + j)),
                pl.BlockSpec((d, 2 * TILE), lambda j: (0, first + j)), pl.BlockSpec((TILE, d), lambda j: (down + j, 0))]
    args = [dh, bt, gu, w, wd]
    if carried:
        in_specs.append(_whole((tokens, d)))
        args.append(given)
    if final:
        in_specs.append(_whole((tokens, d)))
        args.append(h)
    n = count * TILE
    return pl.pallas_call(
        functools.partial(_hidden_back_kernel, carried=carried, final=final),
        grid=(count,),
        in_specs=in_specs,
        out_specs=[pl.BlockSpec((d, 2 * TILE), lambda j: (0, j)), _whole((tokens, d))],
        out_shape=[jax.ShapeDtypeStruct((d, 2 * n + room), BF16), jax.ShapeDtypeStruct((tokens, d), BF16 if final else F32)],
        scratch_shapes=[pltpu.VMEM((tokens, 2 * TILE), BF16)] + ([pltpu.VMEM((tokens, d), F32)] if final else []),
        compiler_params=_params("arbitrary"),
        cost_estimate=_cost(10 * tokens * d * n, 8 * tokens * n + 10 * d * n + 6 * tokens * d, tokens * n),
        name="hidden_back",
    )(*args)


def _alternate_kernel(a_ref, b_ref, out_ref):
    for n in range(a_ref.shape[1] // TILE):
        at = n * TILE
        out_ref[:, 2 * at : 2 * at + TILE] = a_ref[:, at : at + TILE]
        out_ref[:, 2 * at + TILE : 2 * at + 2 * TILE] = b_ref[:, at : at + TILE]


def alternate(a, b, number, parts, k):
    _, rows, ff = a.shape
    wide = ff // 2
    count = 2 // parts
    return pl.pallas_call(
        _alternate_kernel,
        grid=(count,),
        in_specs=[pl.BlockSpec((None, rows, wide), lambda j: (number, 0, k * count + j))] * 2,
        out_specs=pl.BlockSpec((rows, 2 * wide), lambda j: (0, j)),
        out_shape=jax.ShapeDtypeStruct((rows, 2 * wide * count), a.dtype),
        compiler_params=_params("arbitrary"),
        cost_estimate=_cost(rows * ff, 8 * rows * ff // parts),
        name="alternate",
    )(a, b)


def _part_kernel(*refs, layers):
    *ins, gate_ref, up_ref, out_ref = refs
    rows, d = ins[0].shape[0], out_ref.shape[2]
    for n in range(layers):
        for k, ref in enumerate((ins[n], ins[layers + n])):
            half = ins[n].shape[1] // 2
            for at in range(0, half, TILE):
                gate_ref[n, :, k * half + at : k * half + at + TILE] = ref[:, 2 * at : 2 * at + TILE]
                up_ref[n, :, k * half + at : k * half + at + TILE] = ref[:, 2 * at + TILE : 2 * at + 2 * TILE]
        ref, base = ins[layers + n], ins[n].shape[1]
        out_ref[n, :rows, :] = ref[:, base : base + d]
        extra, wide = out_ref.shape[1] - rows, ref.shape[1] - base - d
        for m in range(d // wide):
            out_ref[n, rows:, m * wide : (m + 1) * wide] = ref[m * extra : (m + 1) * extra, base + d :]


def part(firsts, seconds, out_rows):
    rows, both = firsts[0].shape
    d = rows * (seconds[0].shape[1] - both) // out_rows
    layers = len(firsts)
    shapes = [(layers, rows, both), (layers, rows, both), (layers, out_rows, d)]
    return pl.pallas_call(
        functools.partial(_part_kernel, layers=layers),
        in_specs=[pl.BlockSpec(memory_space=pltpu.VMEM)] * (2 * layers),
        out_specs=[pl.BlockSpec(memory_space=pltpu.VMEM)] * 3,
        out_shape=[jax.ShapeDtypeStruct(shape, BF16) for shape in shapes],
        compiler_params=pltpu.CompilerParams(vmem_limit_bytes=VMEM),
        cost_estimate=_cost(rows * both, 8 * rows * both * layers),
        name="part",
    )(*firsts, *seconds)


def _thirds_kernel(*refs, layers):
    for n in range(layers):
        for m, out_ref in enumerate(refs[layers:]):
            width = out_ref.shape[2]
            out_ref[n] = refs[n][:, m * width : (m + 1) * width]


def thirds(sums):
    (rows, width), layers = sums[0].shape, len(sums)
    return pl.pallas_call(
        functools.partial(_thirds_kernel, layers=layers),
        in_specs=[pl.BlockSpec(memory_space=pltpu.VMEM)] * layers,
        out_specs=[pl.BlockSpec(memory_space=pltpu.VMEM)] * 3,
        out_shape=[jax.ShapeDtypeStruct((layers, rows, width // 3), BF16)] * 3,
        compiler_params=pltpu.CompilerParams(vmem_limit_bytes=VMEM),
        cost_estimate=_cost(rows * width, 4 * rows * width * layers),
        name="thirds",
    )(*sums)


def _out_back_kernel(d_ref, o_ref, w_ref, _, do_ref, dw_ref, *, per):
    for r in _pieces(d_ref.shape[0]):
        do_ref[r, :] = _dot(d_ref[r, :], w_ref[...], 1, 1).astype(BF16)
    got = _dot(o_ref[...].T, d_ref[...], 1, 0).astype(BF16)
    rows, d = dw_ref.shape[0] // per, d_ref.shape[1]
    held, wide = got.shape[0] // per, dw_ref.shape[1] - d
    for k in range(per):
        dw_ref[k * rows : (k + 1) * rows, :d] = got[k * held : k * held + rows, :]
        for m in range(d // wide):
            extra = held - rows
            at = k * rows + m * extra
            dw_ref[at : at + extra, d:] = got[k * held + rows : (k + 1) * held, m * wide : (m + 1) * wide]


def out_back(d_h, o, w, dw, group):
    tokens, d = d_h.shape
    width = o.shape[1]
    rows, per = d // group, HEAD * group // width
    last = dw.shape[1] // width - 1
    return pl.pallas_call(
        functools.partial(_out_back_kernel, per=per),
        grid=(width // HEAD,),
        in_specs=[_whole((tokens, d)), pl.BlockSpec((tokens, HEAD), lambda j: (0, j)), pl.BlockSpec((HEAD, d), lambda j: (j, 0)),
                  pl.BlockSpec(memory_space=pl.ANY)],
        out_specs=[pl.BlockSpec((tokens, HEAD), lambda j: (0, j)), pl.BlockSpec((per * rows, width), lambda j: (j, last))],
        out_shape=[jax.ShapeDtypeStruct((tokens, width), BF16), jax.ShapeDtypeStruct(dw.shape, BF16)],
        input_output_aliases={3: 1},
        compiler_params=_params("arbitrary"),
        cost_estimate=_cost(4 * tokens * d * width, 2 * (tokens * d + 2 * tokens * width + 2 * d * width)),
        name="out_back",
    )(d_h, o, w, dw)


def _gap(bk):
    return lax.broadcasted_iota(jnp.int32, (bk, bk), 1) - lax.broadcasted_iota(jnp.int32, (bk, bk), 0)


def _blocks(block, pieces, iq, bq, bk):
    first = iq * (bq // bk)
    lax.fori_loop(0, first, lambda j, _: block(j, pieces, -1), None)
    for n in range(bq // bk):
        block(first + n, [(i, at) for i, at in pieces if at >= n * bk], n * bk)


def _attend_kernel(q_ref, k_ref, v_ref, o_ref, lse_ref, top_s, mix_s, gap_s, *, kb, bq, bk):
    d = HEAD
    iq = pl.program_id(1)
    scale = d**-0.5
    e = scale * LOG2E
    wide = bk
    pieces = [(i, at) for i in range(kb) for at in range(0, bq, wide)]

    @pl.when(iq == 0)
    def _():
        gap_s[...] = _gap(bk)

    for i in range(kb):
        top_s[i : i + 1, :] = jnp.full((1, bq), NEG, F32)
        mix_s[i] = jnp.zeros((d + 8, bq), F32)
    ones = jnp.ones((8, bk), BF16)

    def block(j, pieces, cut):
        here = pl.ds(j * bk, bk)
        scores = [_dot(k_ref[here, i * d : (i + 1) * d], q_ref[at : at + wide, i * d : (i + 1) * d], 1, 1) for i, at in pieces]
        ok = gap_s[...] >= 0 if cut >= 0 else None
        weights, keeps = [], []
        for (i, at), s in zip(pieces, scores):
            if at == cut:
                s = jnp.where(ok, s, HIDDEN)
            old = top_s[i : i + 1, at : at + wide]
            top = jnp.maximum(old, s.max(axis=0, keepdims=True))
            top_s[i : i + 1, at : at + wide] = top
            weights.append(jnp.exp2((s - top) * e).astype(BF16))
            keeps.append(jnp.exp2((old - top) * e))
        for (i, at), p, keep in zip(pieces, weights, keeps):
            values = jnp.concatenate([v_ref[here, i * d : (i + 1) * d].T, ones], axis=0)
            mix_s[i, :, at : at + wide] = mix_s[i, :, at : at + wide] * keep + _dot(values, p, 1, 0)

    _blocks(block, pieces, iq, bq, bk)
    for i in range(kb):
        top, total = top_s[i : i + 1, :], mix_s[i, d : d + 1, :]
        o_ref[:, i * d : (i + 1) * d] = (mix_s[i, :d, :] * (1 / total)).T.astype(o_ref.dtype)
        lse_ref[i] = top * scale + jnp.log(total)


def attend(qkv, width):
    tokens = qkv.shape[0]
    kb, bq, bk = width // HEAD, 1024, 512
    wide = kb * HEAD
    n = width // wide
    return pl.pallas_call(
        functools.partial(_attend_kernel, kb=kb, bq=bq, bk=bk),
        grid=(n, tokens // bq),
        in_specs=[pl.BlockSpec((bq, wide), lambda ih, iq: (iq, ih)), pl.BlockSpec((tokens, wide), lambda ih, iq: (0, n + ih)),
                  pl.BlockSpec((tokens, wide), lambda ih, iq: (0, 2 * n + ih))],
        out_specs=[pl.BlockSpec((bq, wide), lambda ih, iq: (iq, ih)), pl.BlockSpec((kb, 1, bq), lambda ih, iq: (ih, 0, iq))],
        out_shape=[jax.ShapeDtypeStruct((tokens, width), BF16), jax.ShapeDtypeStruct((width // HEAD, 1, tokens), F32)],
        scratch_shapes=[pltpu.VMEM((kb, bq), F32), pltpu.VMEM((kb, HEAD + 8, bq), F32), pltpu.VMEM((bk, bk), jnp.int32)],
        compiler_params=_params("arbitrary", "arbitrary"),
        cost_estimate=_cost(4 * width * tokens * tokens, 8 * tokens * width, width // HEAD * tokens * tokens),
        name="attend",
    )(qkv, qkv, qkv)


def _unturn(t, cos, sin):
    half = t.shape[1] // 2
    t = t.astype(BF16).astype(F32)
    a, b = t[:, :half], t[:, half:]
    return jnp.concatenate([(a * cos + b * sin).astype(BF16), (b * cos - a * sin).astype(BF16)], axis=1)


def _attend_back_kernel(q_ref, k_ref, v_ref, o_ref, do_ref, lse_ref, cos_ref, sin_ref, dq_ref, dk_ref, dv_ref, dq_s, dk_s, dv_s, gap_s,
                        *, kb, bq, bk):
    d = HEAD
    iq = pl.program_id(1)
    scale = d**-0.5
    e = scale * LOG2E
    wide = bk
    pieces = [(i, at) for i in range(kb) for at in range(0, bq, wide)]

    @pl.when(iq == 0)
    def _():
        gap_s[...] = _gap(bk)
        dk_s[...] = jnp.zeros_like(dk_s)
        dv_s[...] = jnp.zeros_like(dv_s)

    dq_s[...] = jnp.zeros_like(dq_s)
    lses = [lse_ref[i] * LOG2E for i in range(kb)]
    deltas = []
    for i in range(kb):
        both = do_ref[:, i * d : (i + 1) * d].astype(F32) * o_ref[:, i * d : (i + 1) * d].astype(F32)
        deltas.append((both[:, : d // 2] + both[:, d // 2 :]).T.sum(axis=0, keepdims=True))

    def block(j, pieces, cut):
        here = pl.ds(j * bk, bk)
        qs = [q_ref[at : at + wide, i * d : (i + 1) * d] for i, at in pieces]
        dos = [do_ref[at : at + wide, i * d : (i + 1) * d] for i, at in pieces]
        scores = [_dot(k_ref[here, i * d : (i + 1) * d], x, 1, 1) for (i, _), x in zip(pieces, qs)]
        dps = [_dot(v_ref[here, i * d : (i + 1) * d], x, 1, 1) for (i, _), x in zip(pieces, dos)]
        ok = gap_s[...] >= 0 if cut >= 0 else None
        for n, (i, at) in enumerate(pieces):
            p = jnp.exp2(scores[n] * e - lses[i][:, at : at + wide])
            if at == cut:
                p = jnp.where(ok, p, 0.0)
            ds = (p * (dps[n] - deltas[i][:, at : at + wide])).astype(BF16)
            dv_s[i, here, :] += _dot(p.astype(BF16), dos[n], 1, 0)
            dk_s[i, here, :] += _dot(ds, qs[n], 1, 0)
            dq_s[i, :, at : at + wide] += _dot(k_ref[here, i * d : (i + 1) * d].T, ds, 1, 0)

    _blocks(block, pieces, iq, bq, bk)
    here = pl.ds(iq * bq, bq)
    for i in range(kb):
        dq_ref[:, i * d : (i + 1) * d] = _unturn((dq_s[i] * scale).T, cos_ref[here, :], sin_ref[here, :])

    @pl.when(iq == pl.num_programs(1) - 1)
    def _():
        for i in range(kb):
            for r in _pieces(dk_ref.shape[0]):
                dk_ref[r, i * d : (i + 1) * d] = _unturn(dk_s[i, r, :] * scale, cos_ref[r, :], sin_ref[r, :])
                dv_ref[r, i * d : (i + 1) * d] = dv_s[i, r, :].astype(BF16)


def attend_back(qkv, o, do, lse, cos, sin):
    tokens, width = o.shape
    kb, bq, bk = 2, 1024, 512
    wide = kb * HEAD
    n = width // wide
    queries = pl.BlockSpec((bq, wide), lambda ih, iq: (iq, ih))
    keys = pl.BlockSpec((tokens, wide), lambda ih, iq: (0, ih))
    return pl.pallas_call(
        functools.partial(_attend_back_kernel, kb=kb, bq=bq, bk=bk),
        grid=(n, tokens // bq),
        in_specs=[queries, pl.BlockSpec((tokens, wide), lambda ih, iq: (0, n + ih)), pl.BlockSpec((tokens, wide), lambda ih, iq: (0, 2 * n + ih)),
                  queries, queries, pl.BlockSpec((kb, 1, bq), lambda ih, iq: (ih, 0, iq)), _whole(cos.shape), _whole(sin.shape)],
        out_specs=[queries, keys, keys],
        out_shape=[jax.ShapeDtypeStruct((tokens, width), BF16)] * 3,
        scratch_shapes=[pltpu.VMEM((kb, HEAD, bq), F32), pltpu.VMEM((kb, tokens, HEAD), F32), pltpu.VMEM((kb, tokens, HEAD), F32),
                        pltpu.VMEM((bk, bk), jnp.int32)],
        compiler_params=_params("arbitrary", "arbitrary"),
        cost_estimate=_cost(10 * width * tokens * tokens, 16 * tokens * width, width // HEAD * tokens * tokens),
        name="attend_back",
    )(qkv, qkv, qkv, o, do, lse, cos, sin)


def matmul(a, w):
    return jnp.dot(a, w, preferred_element_type=F32).astype(BF16)


def outer(a, b):
    return _dot(a, b, 0, 0).astype(BF16)


def solution(mesh):
    gather = lambda w: lax.all_gather(w, "dp", axis=0, tiled=True)
    scatter = lambda w: lax.psum_scatter(w, "dp", scatter_dimension=0, tiled=True)
    group = mesh.shape["dp"]

    def step(x, dy, wq, wk, wv, wo, w_gate, w_up, w_down):
        layers, rows, width = wq.shape
        d, ff = wo.shape[2], w_gate.shape[2]
        h, dh = x[0], dy[0]
        tokens = h.shape[0]
        half = HEAD // 2
        angle = jnp.arange(tokens, dtype=F32)[:, None] * THETA ** (-jnp.arange(half, dtype=F32) / half)
        cos, sin = jnp.cos(angle), jnp.sin(angle)

        def hold(value, after):
            return value if after is None else lax.optimization_barrier((value, after))[0]

        kept, before = [], None
        for number in range(layers):
            later = lambda value: value if number else None
            qkvo = gather(hold(jnp.concatenate([wq[number], wk[number], wv[number], wo[number].reshape(rows, width)], axis=1), before))
            parts = 2 if number == layers - 1 else 1
            both = [alternate(w_gate, w_up, number, parts, k) for k in range(parts)]
            both[0] = gather(hold(both[0], later(h)))
            out = qkvo[:, 3 * width :].reshape(width, d)
            qkv, at = project(h, qkvo, cos, sin, width)
            both[1:] = [gather(hold(b, later(qkv))) for b in both[1:]]
            o, lse = attend(qkv, width)
            mid = h + matmul(o, out)
            down = gather(hold(w_down[number], later(mid)))
            gu, act, bt = gate_up(mid, both[0], ff)
            gus = [gu]
            if len(both) > 1:
                gu, act = gate_up(mid, both[1], ff, act)
                gus.append(gu)
            kept.append((h, qkvo, both, down, out, qkv, at, o, lse, mid, gus, act, bt))
            before = act
            h = mid + matmul(act, down)

        by_down, by_qkv, first, second = ([None] * layers for _ in range(4))
        tiles = ff // TILE
        cut = tiles // 2
        sent = []

        def tie(*values, count=None):
            now = sent[:count]
            out = lax.optimization_barrier((*values, *(store[n] for store, n in now)))
            for (store, n), got in zip(now, out[len(values) :]):
                store[n] = got
            del sent[: len(now)]
            return out[: len(values)]

        def send(store, n, value):
            store[n] = scatter(value)
            sent.append((store, n))

        for number in reversed(range(layers)):
            h, qkvo, both, down, out, qkv, at, o, lse, mid, gus, act, bt = kept[number]
            by_w, dh = lax.optimization_barrier((outer(act, dh), dh))
            send(by_down, number, by_w)
            by_w, given = hidden_back(dh, bt, gus[0], both[0], down, 0, 0, cut)
            (given,) = tie(given)
            send(first, number, by_w)
            at_b = 0 if len(both) > 1 else cut
            by_w, d_mid = hidden_back(dh, bt, gus[-1], both[-1], down, at_b, cut, tiles - cut, room=width, given=given, h=mid)
            (d_mid,) = tie(d_mid)
            do, by_w = out_back(d_mid, o, out, by_w, group)
            send(second, number, by_w)
            parts = attend_back(qkv, o, do, lse, cos, sin)
            by_w, *parts = tie(project_weights(at, parts), *parts)
            send(by_qkv, number, by_w)
            dh = project_input(h, d_mid, qkvo, parts)
        by_gate, by_up, by_out = part(first, second, width // group)
        return dh[None], *thirds(by_qkv), by_out, by_gate, by_up, jnp.stack(by_down)

    states, cut = P(("rep", "dp"), None, None), P(None, "dp", None)
    return jax.shard_map(
        step,
        mesh=mesh,
        in_specs=(states, states) + (cut,) * 7,
        out_specs=(states,) + (P("rep", "dp", None),) * 7,
        check_vma=False,
    )
```
